32 devices in a mesh: dp: 2 (over z, core), tp: 16 (over x, y).
Axes of the slice: x: 4, y: 4, z: 1, core: 2. Of those that a mesh axis runs over, the one named last changes fastest.
The devices are a block of a 4x4x8 slice.
Arguments:
- x: bfloat16 [11264, 3072], P(('dp', 'tp')), parts along dimension 0
- w_gate: bfloat16 [3072, 24576], P(None, 'tp')
- w_up: bfloat16 [3072, 24576], P(None, 'tp')
- w_down: bfloat16 [24576, 3072], P('tp')
Outputs:
- output: bfloat16 [11264, 3072], P(('dp', 'tp')), parts along dimension 0
There are 2 independent parts. The reference program is written for one: setup_inputs(seed, part) draws one part's arguments, and reference() takes and returns one part's arrays. A program takes and returns all parts, laid end to end along the dimension named above; an argument that names none is the same for every part.
All inputs are finite; a program needn't handle non-finite values.
Results may differ from the reference program's by a relative error of at most 0.016.
Values are sent between devices in bfloat16 or wider.
A program may use at most 768 MiB of HBM per device.

```python
import jax
import jax.numpy as jnp

ROWS = 5632
D = 3072
FF = 24576


def setup_inputs(seed: int = 0, part: int = 0) -> dict:
    kx, kg, ku, kd = jax.random.split(jax.random.key(seed), 4)
    drawn = {
        "x": jax.random.normal(jax.random.fold_in(kx, part), (ROWS, D), jnp.float32),
        "w_gate": jax.random.normal(kg, (D, FF), jnp.float32) * D**-0.5,
        "w_up": jax.random.normal(ku, (D, FF), jnp.float32) * D**-0.5,
        "w_down": jax.random.normal(kd, (FF, D), jnp.float32) * FF**-0.5,
    }
    return {k: v.astype(jnp.bfloat16) for k, v in drawn.items()}


def reference(x, w_gate, w_up, w_down):
    gate = jnp.dot(x, w_gate, preferred_element_type=jnp.float32)
    up = jnp.dot(x, w_up, preferred_element_type=jnp.float32)
    hidden = (jax.nn.gelu(gate) * up).astype(jnp.bfloat16)
    return jnp.dot(hidden, w_down, preferred_element_type=jnp.float32).astype(jnp.bfloat16)
```

```python
import functools
import math

import jax
import jax.numpy as jnp
from jax import lax
from jax.experimental import pallas as pl
from jax.experimental.pallas import tpu as pltpu
from jax.sharding import PartitionSpec as P

MESH = pl.DeviceIdType.MESH
TILE = 256
STAGE = 5
LOADS = 3
STAGE_MORE = 11

HALF_US, HOP_US, GATE_US, DOWN_US, LOAD_US = 23.6, 2.0, 8.6, 2.6, 2.0

BLOCKS = [
    (0, 0), (1, 0), (-1, 0), (0, 1), (0, -1), (1, 1), (1, -1), (-1, 1), (-1, -1),
    (2, 0), (0, 2), (2, 1), (1, 2), (2, -1), (-1, 2), (2, 2),
]
SLOT = {b: i for i, b in enumerate(BLOCKS)}
COL = {1: 0, -1: 1}


def norm(o):
    return (o + 1) % 4 - 1


def place(h, first, second):
    a, b = norm(first), norm(second)
    return SLOT[(a, b) if h == 0 else (b, a)]


def gather_plan():
    plan = {}
    for h in (0, 1):
        f, s = h, 1 - h
        for d in (1, -1):
            plan["g1", h, d] = (f, d, 1.0, place(h, 0, 0), place(h, -d, 0), h, None, [])
        for d in (1, -1):
            for o in (0, -1, 1):
                needs = [("g1", h, -o)] if o else []
                plan["g3", h, o, d] = (s, d, 1.0, place(h, o, 0), place(h, o, -d), h, None, needs)
        for d in (1, -1):
            plan["g2", h, d] = (f, d, 0.5, place(h, -d, 0), place(h, 2, 0), h, COL[d], [("g1", h, d)])
        for d in (1, -1):
            for e in (1, -1):
                plan["g3", h, 2, e, d] = (
                    s, d, 0.5, place(h, 2, 0), place(h, 2, -d), h, COL[e], [("g2", h, e)],
                )
            for o in (0, -1, 1):
                plan["g4", h, o, d] = (
                    s, d, 0.5, place(h, o, -d), place(h, o, 2), h, COL[d], [("g3", h, o, d)],
                )
            plan["g4", h, 2, d] = (s, d, 0.5, place(h, 2, -d), place(h, 2, 2), h, COL[d], [("g3", h, 2, d, d)])
    return plan


def scatter_plan():
    steps = {}
    for h in (0, 1):
        u, v = 1 - h, h

        def slot(uo, vo):
            return SLOT[(vo, uo) if h == 0 else (uo, vo)]

        for vo in (-1, 0, 1, 2):
            steps["A", h, vo] = (slot(2, vo), h, [], [(("A", h, vo, d), u, d, d) for d in (1, -1)])
            for d in (1, -1):
                steps["B", h, vo, d] = (
                    slot(d, vo), h, [(("A", h, vo, d), d)], [(("B", h, vo, d), u, d, 0)],
                )
        both = lambda vo: [(("B", h, vo, 1), 0), (("B", h, vo, -1), 0)]
        steps["D", h] = (slot(0, 2), h, both(2), [(("D", h, d), v, d, d) for d in (1, -1)])
        for d in (1, -1):
            steps["E", h, d] = (slot(0, d), h, both(d) + [(("D", h, d), d)], [(("E", h, d), v, d, 0)])
        steps["F", h] = (slot(0, 0), h, both(0) + [(("E", h, 1), 0), (("E", h, -1), 0)], [])
    return steps


def sequence():
    seq = []
    for i, (dx, dy) in enumerate(BLOCKS):
        seq.append(("G", i))
        if dy == 2:
            seq.append(("A", 0, dx))
        if dx == 2:
            seq.append(("A", 1, dy))
    for vo in (1, 2, -1):
        seq += [("B", h, vo, d) for h in (0, 1) for d in (1, -1)]
    seq += [("D", h) for h in (0, 1)]
    seq += [("B", h, 0, d) for h in (0, 1) for d in (1, -1)]
    seq += [("E", h, d) for h in (0, 1) for d in (1, -1)]
    return seq + [("F", h) for h in (0, 1)]


def schedule():
    gather, steps, seq = gather_plan(), scatter_plan(), sequence()
    pieces = {}
    for name, (_, _, _, _, target, _, _, _) in gather.items():
        pieces.setdefault(target, []).append(name)
    link, arrival, actions = {}, {}, []
    waited, issued, loaded, ready = set(), set(), {}, {}
    now = 0.0

    def send(name, axis, d, size):
        start = max(now, link.get((axis, d), 0.0))
        link[axis, d] = start + size * HALF_US
        arrival[name] = link[axis, d] + HOP_US

    def wait(name):
        if name not in waited:
            waited.add(name)
            actions.append(("wait", name))

    def here(names):
        return all(n in arrival and arrival[n] <= now for n in names)

    free = list(range(LOADS))
    stage = [(i, None) for i in range(STAGE)]
    last_gate = max(i for i, item in enumerate(seq) if item[0] == "G")
    at = 0
    done_gates = 0
    while at < len(seq):
        for name, (axis, d, size, _, _, _, _, needs) in gather.items():
            if name not in issued and here(needs):
                issued.add(name)
                for n in needs:
                    wait(n)
                actions.append(("gather", name))
                send(name, axis, d, size)
        for item in seq[at : at + 3]:
            if item in loaded:
                continue
            if item[0] == "G":
                need = pieces.get(item[1], [])
                if item[1] - done_gates > 1 or not here(need):
                    break
                for n in need:
                    wait(n)
                actions.append(("fetch", item[1]))
                loaded[item], ready[item] = [], now + LOAD_US
            else:
                loads = steps[item][2]
                if len(loads) > len(free) or not here([n for n, _ in loads]):
                    break
                taken = []
                for n, rows in loads:
                    wait(n)
                    r = free.pop(0)
                    taken.append((r, n, rows))
                    actions.append(("load", r, n, rows))
                loaded[item], ready[item] = taken, (now + LOAD_US if loads else now)
        item = seq[at]
        if item in loaded and ready[item] <= now:
            if item[0] == "G":
                actions.append(("gate", item[1]))
                now += GATE_US
                done_gates += 1
            else:
                slot, before = stage.pop(0)
                if before is not None:
                    for n in before:
                        now = max(now, arrival[n])
                        actions.append(("sent", n))
                actions.append(("down", item, slot, loaded[item]))
                now += DOWN_US
                free += [r for r, _, _ in loaded[item]]
                sends = steps[item][3]
                for n, axis, d, rows in sends:
                    send(n, axis, d, 0.5 if rows else 1.0)
                stage.append((slot, [n for n, _, _, _ in sends]))
            if at == last_gate:
                more = [(STAGE + i, None) for i in range(STAGE_MORE)]
                stage = more + stage
                free += list(range(LOADS, LOADS + 16 - STAGE_MORE))
            at += 1
            continue
        later = [t for t in arrival.values() if t > now] + [t for t in ready.values() if t > now]
        now = min(later)
    return actions, now, max(link.values())


def kernel(
    side, x_ref, wg_ref, wu_ref, wd_ref, y_ref, ag, ra, rb, rd, re,
    wg, wu, wd, hid, xbuf, rbuf, sbuf, gs, gr, ss, sr, ws, xs, ls, os,
):
    rows, dim = x_ref.shape
    ff = wg_ref.shape[1]
    half, wide = rows // 2, dim // 2
    me = lax.axis_index("tp")
    mx, my = me // side, lax.rem(me, side)

    def peer(axis, d):
        if axis == 0:
            return {"tp": lax.rem(mx + d + side, side) * side + my}
        return {"tp": mx * side + lax.rem(my + d + side, side)}

    barrier = pltpu.get_barrier_semaphore()
    for axis in (0, 1):
        for d in (1, -1):
            pl.semaphore_signal(barrier, inc=1, device_id=peer(axis, d), device_id_type=MESH)
    pl.semaphore_wait(barrier, 4)

    gather, steps = gather_plan(), scatter_plan()
    actions, _, _ = schedule()
    gather_id = {n: i for i, n in enumerate(gather)}
    scatter_id, scatter_send = {}, {}
    for item, (_, _, _, sends) in steps.items():
        for n, axis, d, part in sends:
            scatter_id[n] = len(scatter_id)
            scatter_send[n] = (axis, d, part)

    def span(part):
        return slice(None) if part == 0 else (pl.ds(0, half) if part == 1 else pl.ds(half, half))

    def landing(n):
        d = 0 if n[-1] == 1 else 1
        if n[0] == "A":
            return ra.at[n[1], d, n[2] % 4]
        if n[0] == "B":
            return rb.at[n[1], d, n[2] % 4]
        return (rd if n[0] == "D" else re).at[n[1], d]

    def piece(slot, h, col):
        source = x_ref if slot == 0 else ag.at[slot - 1]
        r = pl.ds(h * half, half)
        return source.at[r] if col is None else source.at[r, pl.ds(col * wide, wide)]

    def gather_copy(n):
        axis, d, _, source, target, h, col, _ = gather[n]
        return pltpu.make_async_remote_copy(
            src_ref=piece(source, h, col),
            dst_ref=piece(target, h, col),
            send_sem=gs.at[gather_id[n]],
            recv_sem=gr.at[gather_id[n]],
            device_id=peer(axis, d),
            device_id_type=MESH,
        )

    def stage_ref(slot):
        if slot < STAGE:
            return sbuf.at[slot]
        return spare(slot - STAGE)

    def spare(i):
        return (wg if i < 8 else wu).at[pl.ds((i % 8) * rows, rows)]

    def load_ref(r):
        return rbuf.at[r] if r < LOADS else spare(STAGE_MORE + r - LOADS)

    slot_of_send = {}

    def scatter_copy(n):
        axis, d, part = scatter_send[n]
        return pltpu.make_async_remote_copy(
            src_ref=stage_ref(slot_of_send[n]).at[span(part)],
            dst_ref=landing(n),
            send_sem=ss.at[scatter_id[n]],
            recv_sem=sr.at[scatter_id[n]],
            device_id=peer(axis, d),
            device_id_type=MESH,
        )

    def received(n):
        if n in gather:
            gather_copy(n).wait_recv()
        else:
            axis, d, part = scatter_send[n]
            pltpu.make_async_remote_copy(
                src_ref=landing(n),
                dst_ref=landing(n),
                send_sem=ss.at[scatter_id[n]],
                recv_sem=sr.at[scatter_id[n]],
                device_id=peer(axis, d),
                device_id_type=MESH,
            ).wait_recv()

    def load_copy(r, n, part):
        return pltpu.make_async_copy(landing(n), load_ref(r).at[span(part)], ls.at[r])

    def fetch_copy(slot, b):
        source = x_ref if slot == 0 else ag.at[slot - 1]
        return pltpu.make_async_copy(source, xbuf.at[b], xs.at[b])

    def gate(slot, b):
        pltpu.make_async_copy(x_ref, xbuf.at[b], xs.at[b]).wait()

        def tile(j, _):
            c = pl.ds(pl.multiple_of(j * TILE, TILE), TILE)
            g = jnp.dot(xbuf[b], wg[:, c], preferred_element_type=jnp.float32)
            u = jnp.dot(xbuf[b], wu[:, c], preferred_element_type=jnp.float32)
            hid[slot, :, c] = (jax.nn.gelu(g) * u).astype(jnp.bfloat16)
            return 0

        lax.fori_loop(0, ff // TILE, tile, 0)

    def down(item, stage, loads):
        slot, h, _, sends = steps[item]
        for r, n, part in loads:
            load_copy(r, n, part).wait()
        out = stage_ref(stage)

        def tile(j, _):
            c = pl.ds(pl.multiple_of(j * TILE, TILE), TILE)
            c_in = pl.ds(pl.multiple_of(h * wide + j * TILE, TILE), TILE)
            term = jnp.dot(hid[slot], wd[:, c_in], preferred_element_type=jnp.float32)
            for r, _, part in loads:
                if part == 0:
                    term = term + load_ref(r)[:, c].astype(jnp.float32)
            for at, rs in ((1, slice(0, half)), (-1, slice(half, rows))):
                piece_ = term[rs]
                for r, _, part in loads:
                    if part == at:
                        piece_ = piece_ + load_ref(r)[rs, c].astype(jnp.float32)
                out[rs, c] = piece_.astype(jnp.bfloat16)
            return 0

        lax.fori_loop(0, wide // TILE, tile, 0)
        if sends:
            for n, _, _, _ in sends:
                slot_of_send[n] = stage
                scatter_copy(n).start()
        else:
            result_copy(h, stage).start()

    def result_copy(h, stage):
        return pltpu.make_async_copy(stage_ref(stage), y_ref.at[:, pl.ds(h * wide, wide)], os.at[h])

    finished = set()
    result_stage = {}

    def run(action):
        kind = action[0]
        if kind == "wait":
            received(action[1])
        elif kind == "gather":
            gather_copy(action[1]).start()
        elif kind == "fetch":
            fetch_copy(action[1], action[1] % 2).start()
        elif kind == "load":
            load_copy(*action[1:]).start()
        elif kind == "sent":
            scatter_copy(action[1]).wait_send()
            finished.add(action[1])
        else:
            item, stage, loads = action[1:]
            if item[0] == "F":
                result_stage[item[1]] = stage
            down(item, stage, loads)

    before, rest = [[]], []
    for action in actions:
        if action[0] == "gate":
            before.append([])
        else:
            before[-1].append(action)
    rest = before.pop()

    weights = [
        pltpu.make_async_copy(a, b, ws.at[i])
        for i, (a, b) in enumerate(((wg_ref, wg), (wu_ref, wu), (wd_ref, wd)))
    ]
    for action in before[0]:
        run(action)
    for w in weights:
        w.start()
    for w in weights[:2]:
        w.wait()

    def step(s, _):
        for k, todo in enumerate(before):
            if k and todo:

                @pl.when(s == k)
                def _(todo=todo, k=k):
                    if k == 1:
                        weights[2].wait()
                    for action in todo:
                        run(action)

        gate(s, lax.rem(s, 2))
        return 0

    lax.fori_loop(0, len(before), step, 0)
    for action in rest:
        run(action)
    for n in gather:
        gather_copy(n).wait_send()
    for n in scatter_id:
        if n not in finished:
            scatter_copy(n).wait_send()
    for h in (0, 1):
        result_copy(h, result_stage[h]).wait()


def solution(mesh):
    side = math.isqrt(mesh.shape["tp"])

    def step(x, w_gate, w_up, w_down):
        rows, dim = x.shape
        ff = w_gate.shape[1]
        half, wide = rows // 2, dim // 2
        gathers = len(gather_plan())
        scatters = sum(len(s[3]) for s in scatter_plan().values())
        bf16 = jnp.bfloat16
        anywhere = pl.BlockSpec(memory_space=pl.ANY)
        shapes = [
            (rows, dim),
            (15, rows, dim),
            (2, 2, 4, half, wide),
            (2, 2, 4, rows, wide),
            (2, 2, half, wide),
            (2, 2, rows, wide),
        ]
        return pl.pallas_call(
            functools.partial(kernel, side),
            out_shape=[jax.ShapeDtypeStruct(shape, bf16) for shape in shapes],
            in_specs=[anywhere] * 4,
            out_specs=[anywhere] * len(shapes),
            scratch_shapes=[
                pltpu.VMEM((dim, ff), bf16),
                pltpu.VMEM((dim, ff), bf16),
                pltpu.VMEM((ff, dim), bf16),
                pltpu.VMEM((16, rows, ff), bf16),
                pltpu.VMEM((2, rows, dim), bf16),
                pltpu.VMEM((LOADS, rows, wide), bf16),
                pltpu.VMEM((STAGE, rows, wide), bf16),
                pltpu.SemaphoreType.DMA((gathers,)),
                pltpu.SemaphoreType.DMA((gathers,)),
                pltpu.SemaphoreType.DMA((scatters,)),
                pltpu.SemaphoreType.DMA((scatters,)),
                pltpu.SemaphoreType.DMA((3,)),
                pltpu.SemaphoreType.DMA((2,)),
                pltpu.SemaphoreType.DMA((LOADS + 16 - STAGE_MORE,)),
                pltpu.SemaphoreType.DMA((2,)),
            ],
            compiler_params=pltpu.CompilerParams(
                collective_id=0, has_side_effects=True, vmem_limit_bytes=66_000_000
            ),
        )(x, w_gate, w_up, w_down)[0]

    return jax.shard_map(
        step,
        mesh=mesh,
        in_specs=(P(("dp", "tp"), None), P(None, "tp"), P(None, "tp"), P("tp", None)),
        out_specs=P(("dp", "tp"), None),
        check_vma=False,
    )


if __name__ == "__main__":
    acts, end, links = schedule()
    for a in acts:
        print(a)
    print(len(acts), end, links)
```

```python
import functools
import math

import jax
import jax.numpy as jnp
from jax import lax
from jax.experimental import pallas as pl
from jax.experimental.pallas import tpu as pltpu
from jax.sharding import PartitionSpec as P

MESH = pl.DeviceIdType.MESH
TILE = 256
EARLY = 4
STAGE = 12
LOADS = 8

HALF_US, HOP_US, LOAD_US, DOWN_US, CORE_US = 23.4, 2.0, 2.0, 3.2, 2.0
GATE_US = (7.4, 2.5, 2.5, 2.5)

BLOCKS = [(0, 0), (0, 1), (0, -1), (0, 2), (2, 0), (2, 1), (2, -1), (2, 2)]
SLOT = {b: i for i, b in enumerate(BLOCKS)}
UNITS = [
    ((0, 1), (0, -1)), ((1, 1), (2, 1)), ((1, -1), (2, -1)), ((3, 1), (3, -1)),
    ((4, 1), (4, -1)), ((5, 1), (6, 1)), ((5, -1), (6, -1)), ((7, 1), (7, -1)),
]
GATES = [
    (0, 0, 5), (1, 0, 4), (0, 5, 6), (1, 4, 7), (2, 0, 1), (0, 6, 7), (2, 1, 8), (1, 7, 8),
    (0, 7, 8), (3, 0, 8),
]
STEPS = [
    ("A", 0, 2), ("B", 0, 0, -1), ("B", 0, 0, 1), ("X", 2), ("X", -1), ("B", 0, 2, -1),
    ("B", 0, 2, 1), ("A", 1, 2), ("X", 1), ("A", 1, 0), ("C", 0), ("A", 2, 0),
    ("X", 0), ("B", 1, 2, -1), ("B", 1, 2, 1), ("B", 2, 0, 1), ("B", 2, 0, -1), ("B", 1, 0, -1),
    ("C", 1), ("B", 1, 0, 1), ("F", 0), ("F", 2), ("F", 1),
]
EARLY_STEPS = [(("G", 3, 4), ("A", 0, 0))]
PIECE = 0.7273
ORDER = ("g1", "u1", "u2", "g2", "g3", "u3", "d0", "d2", "d1")


def transfers():
    plan = {}
    for d in (1, -1):
        plan["x1", d] = (0, d, 1.0, [], None)
        for part in (1, -1):
            plan["y1", 0, d, part] = (1, d, 1.0, [], None)
        plan["g1", d] = (0, d, PIECE, [], None)
    for d in (1, -1):
        plan["x2", d] = (0, d, 1.0, [("x1", d)], None)
        plan["y2", 0, d] = (1, d, 1.0, [("y1", 0, d, d)], None)
    for d in (1, -1):
        for w in ORDER[1:]:
            plan[w, d] = (0, d, PIECE, [], ("x2", d))
    for d in (1, -1):
        for w in ORDER:
            plan["over", w, d] = (2, 0, PIECE, [(w, d)], None)
        for part in (1, -1):
            plan["y1", 2, d, part] = (1, d, 1.0, [("x2", part)], None)
        plan["y2", 2, d] = (1, d, 1.0, [("y1", 2, d, d)], None)
        for t in (0, 1):
            plan["r2", t, 0, d] = (0, d, 1 / 3, [("r1", t, 0, d)], None)
        for dy in (2, 1, -1, 0):
            plan["r2", 2, dy, d] = (0, d, 1 / 3, [("r1", 2, dy, d)], None)
    return plan


def pieces_of(unit):
    names = []
    for slot, part in UNITS[unit]:
        across, dy = BLOCKS[slot]
        if dy == 0:
            names += [("x2", part)] if across else []
        elif dy == 2:
            names.append(("y2", across, part))
        else:
            names.append(("y1", across, -dy, part))
    return names


def weight_names(part):
    names = (f"g{part}", f"u{part}") if part < 4 else (f"d{part - 5}",)
    return [n for w in names for d in (1, -1) for n in ((w, d), ("over", w, d))]


def sums():
    steps = {}
    both = lambda t, e: [(("B", t, e, 1), 0), (("B", t, e, -1), 0)]
    over = lambda t, dy: [(("r2", t, dy, 1), 1), (("r2", t, dy, -1), -1)]
    for t in (0, 1):
        for e in (2, 0):
            steps["A", t, e] = (SLOT[e, 2], t, [], [(("A", t, e, d), 1, d, d) for d in (1, -1)])
            for d in (1, -1):
                steps["B", t, e, d] = (SLOT[e, d], t, [(("A", t, e, d), d)], [(("B", t, e, d), 1, d, 0)])
        steps["C", t] = (SLOT[2, 0], t, both(t, 2), [(("r1", t, 0, d), 0, d, d) for d in (1, -1)])
    for dy in (2, 1, -1, 0):
        steps["X", dy] = (SLOT[2, dy], 2, [], [(("r1", 2, dy, d), 0, d, d) for d in (1, -1)])
    steps["A", 2, 0] = (SLOT[0, 2], 2, over(2, 2), [(("A", 2, 0, d), 1, d, d) for d in (1, -1)])
    for d in (1, -1):
        loads = over(2, d) + [(("A", 2, 0, d), d)]
        steps["B", 2, 0, d] = (SLOT[0, d], 2, loads, [(("B", 2, 0, d), 1, d, 0)])
    for t in (0, 1, 2):
        steps["F", t] = (SLOT[0, 0], t, both(t, 0) + over(t, 0), [])
    return steps


def sequence():
    seq = [("G", part, i) for part, a, b in GATES for i in range(a, b)]
    for at, item in EARLY_STEPS:
        seq.insert(seq.index(at) + 1, item)
    return seq + STEPS


def schedule():
    plan, steps = transfers(), sums()
    seq = sequence()
    link, arrival, actions = {}, {}, []
    waited, issued, loaded, ready, brought = set(), set(), {}, {}, {}
    now = 0.0

    def send(name, axis, d, size):
        start = max(now, link.get((axis, d), 0.0))
        link[axis, d] = start + size * (CORE_US if axis == 2 else HALF_US)
        arrival[name] = link[axis, d] + HOP_US

    def wait(names):
        for name in names:
            if name not in waited:
                waited.add(name)
                actions.append(("wait", name))

    def here(names):
        return all(n in arrival and arrival[n] <= now for n in names)

    free = list(range(LOADS))
    stage = [(i, None) for i in range(EARLY)]
    own_left = sum(b - a for part, a, b in GATES if part == 0)
    gates = 1 + max(i for i, item in enumerate(seq) if item[0] == "G")
    at = fetched = 0
    while at < len(seq):
        for name, (axis, d, size, needs, after) in plan.items():
            if name not in issued and here(needs) and (after is None or after in issued):
                issued.add(name)
                wait(needs)
                actions.append(("go", name))
                send(name, axis, d, size)
        for part in (1, 2, 3, 4, 5, 6, 7):
            if part not in brought:
                names = [] if part == 4 else weight_names(part)
                if here(names) and not (part >= 4 and own_left):
                    wait(names)
                    actions.append(("bring", part))
                    brought[part] = now + 4.0
        for k, item in enumerate(seq[at : at + 3]):
            if item in loaded:
                continue
            if item[0] == "G":
                if k > 1 or not here(pieces_of(item[2])):
                    break
                wait(pieces_of(item[2]))
                actions.append(("fetch", item[2], fetched % 2))
                fetched += 1
                loaded[item], ready[item] = [], now + LOAD_US
            else:
                loads = steps[item][2]
                units = [i for i, u in enumerate(UNITS) if steps[item][0] in (u[0][0], u[1][0])]
                if any(("G", part, i) in seq[at:] for part in range(4) for i in units):
                    break
                if (loads and at < gates) or len(loads) > len(free) or not here([n for n, _ in loads]):
                    break
                wait([n for n, _ in loads])
                taken = []
                for n, rows in loads:
                    taken.append((free.pop(0), n, rows))
                    actions.append(("load", *taken[-1]))
                loaded[item], ready[item] = taken, (now + LOAD_US if loads else now)
        item = seq[at]
        parts = ([item[1]] if item[1] else []) if item[0] == "G" else [4, 5 + steps[item][1]]
        if item in loaded and ready[item] <= now and all(brought.get(q, 1e9) <= now for q in parts):
            if item[0] == "G":
                actions.append(("gate", item[1], item[2]))
                now += GATE_US[item[1]]
                own_left -= item[1] == 0
            else:
                slot, before = stage.pop(0)
                for n in before or []:
                    now = max(now, arrival[n])
                    actions.append(("sent", n))
                actions.append(("down", item, slot, loaded[item]))
                now += DOWN_US
                free += [r for r, _, _ in loaded[item]]
                for n, axis, d, rows in steps[item][3]:
                    send(n, axis, d, 1 / 3 if rows else 2 / 3)
                stage.append((slot, [n for n, _, _, _ in steps[item][3]]))
            at += 1
            if at == gates:
                stage = [(EARLY + i, None) for i in range(STAGE)] + stage
            continue
        now = min(t for t in [*arrival.values(), *ready.values(), *brought.values()] if t > now)
    return actions, now, max(link.values())


def kernel(
    side, x_ref, wg_ref, wu_ref, wd_ref, y_ref, ag, rl, nb, nd, ta, tb, rr, rf,
    w, hid, xbuf, sbuf, ts, tr, ss, sr, ws, xs, ls, os,
):
    rows, dim = x_ref.shape
    ff = wg_ref.shape[1]
    half, wide, third = rows // 2, dim // 2, dim // 3
    quarter = ff // 4
    some = quarter // 3
    me, group = lax.axis_index("tp"), lax.axis_index("dp")
    core = lax.rem(group, 2)
    mx, my = me // side, lax.rem(me, side)

    def peer(axis, d):
        if axis == 0:
            return {"tp": lax.rem(mx + d + side, side) * side + my}
        if axis == 1:
            return {"tp": mx * side + lax.rem(my + d + side, side)}
        return {"dp": group + 1 - 2 * core}

    barrier = pltpu.get_barrier_semaphore()
    for axis, d in ((0, 1), (0, -1), (1, 1), (1, -1), (2, 0)):
        pl.semaphore_signal(barrier, inc=1, device_id=peer(axis, d), device_id_type=MESH)
    pl.semaphore_wait(barrier, 5)

    plan, steps = transfers(), sums()
    actions, _, _ = schedule()
    plan_id = {n: i for i, n in enumerate(plan)}
    sum_id, sum_send = {}, {}
    for _, _, _, sends in steps.values():
        for n, axis, d, part in sends:
            sum_id[n] = len(sum_id)
            sum_send[n] = (axis, d, part)

    def way(d):
        return 0 if d == 1 else 1

    def span(part):
        return slice(None) if part == 0 else pl.ds(0 if part == 1 else half, half)

    def block(slot):
        return x_ref if slot == 0 else ag.at[slot - 1]

    def landing(n):
        d = way(n[-1])
        if n[0] == "A":
            return ta.at[n[1] * 2 + n[2] // 2, d]
        if n[0] == "B":
            return tb.at[n[1] * 2 + n[2] // 2, d]
        return (rr if n[0] == "r1" else rf).at[n[1] + n[2] % 4, d]

    def ends(n):
        kind, d = n[0], n[-1]
        if kind == "x1":
            return x_ref.at[span(d)], rl.at[way(d)]
        if kind == "x2":
            return rl.at[way(d)], block(SLOT[2, 0]).at[span(d)]
        if kind == "y1":
            _, e, d, part = n
            return block(SLOT[e, 0]).at[span(part)], block(SLOT[e, -d]).at[span(part)]
        if kind == "y2":
            e = n[1]
            return block(SLOT[e, -d]).at[span(d)], block(SLOT[e, 2]).at[span(d)]
        if kind == "r2":
            return landing(("r1", *n[1:])), landing(n)
        over = kind == "over"
        name = n[1] if over else kind
        number = int(name[1])
        if name[0] == "d":
            buf = nd.at[number, way(d)]
        else:
            buf = nb.at[number - 1, 0 if name[0] == "g" else 1, way(d)]
        if over:
            return buf.at[0], buf.at[1]
        at = (2 * quarter if d == 1 else 0) + quarter * core
        if name[0] == "d":
            start = pl.multiple_of(at, quarter)
            return wd_ref.at[pl.ds(start, quarter), pl.ds(number * third, third)], buf.at[0]
        start = pl.multiple_of(at + (number - 1) * some, some)
        return (wg_ref if name[0] == "g" else wu_ref).at[:, pl.ds(start, some)], buf.at[0]

    def moving(n):
        axis, d = plan[n][:2]
        source, target = ends(n)
        return pltpu.make_async_remote_copy(
            src_ref=source, dst_ref=target, send_sem=ts.at[plan_id[n]], recv_sem=tr.at[plan_id[n]],
            device_id=peer(axis, d), device_id_type=MESH,
        )

    def spare(i):
        if i < EARLY:
            return sbuf.at[i]
        i -= EARLY
        return w.at[2 + i // 8, pl.ds((i % 8) * rows, rows), pl.ds(0, third)]

    def load_ref(r):
        if r < 4:
            return spare(EARLY + STAGE + r)
        return xbuf.at[r // 2 - 2, :, pl.ds((r % 2) * wide, third)]

    slot_of = {}

    def leaving(n, source):
        axis, d, part = sum_send[n]
        return pltpu.make_async_remote_copy(
            src_ref=source, dst_ref=landing(n), send_sem=ss.at[sum_id[n]], recv_sem=sr.at[sum_id[n]],
            device_id=peer(axis, d), device_id_type=MESH,
        )

    def staged(n):
        return leaving(n, spare(slot_of[n]).at[span(sum_send[n][2])])

    def load_copy(r, n, part):
        return pltpu.make_async_copy(landing(n), load_ref(r).at[span(part)], ls.at[r])

    def bring(part):
        copies = []
        if part == 4:
            for h in (0, 1):
                copies.append((wd_ref.at[:, pl.ds(h * wide, wide)], w.at[0, pl.ds(h * ff, ff)]))
        elif part < 4:
            for p in range(4):
                for i in (0, 1):
                    target = w.at[2 + i, :, pl.ds(((part - 1) * 4 + p) * some, some)]
                    copies.append((nb.at[part - 1, i, p // 2, p % 2], target))
        else:
            t = part - 5
            for h in (0, 1):
                lo, hi = max(t * third, h * wide), min((t + 1) * third, (h + 1) * wide)
                if lo < hi:
                    for p in range(4):
                        source = nd.at[t, p // 2, p % 2, :, pl.ds(lo - t * third, hi - lo)]
                        target = w.at[1, pl.ds(h * ff + p * quarter, quarter), pl.ds(lo - h * wide, hi - lo)]
                        copies.append((source, target))
        base = {1: 2, 2: 10, 3: 18, 4: 26, 5: 28, 6: 32, 7: 40}[part]
        return [pltpu.make_async_copy(s, t, ws.at[base + i]) for i, (s, t) in enumerate(copies)]

    def gate_tiles(part, slot, b):
        pltpu.make_async_copy(x_ref, xbuf.at[b], xs.at[b]).wait()
        first, last = (0, ff // TILE) if part == 0 else (0, 4 * some // TILE)
        at = 2 if part else 0

        def pair(i, _):
            for j in (2 * i, 2 * i + 1):
                c = pl.ds(pl.multiple_of((4 * some * (part - 1) if part else 0) + j * TILE, TILE), TILE)
                g = jnp.dot(xbuf[b], w[at, :, c], preferred_element_type=jnp.float32)
                u = jnp.dot(xbuf[b], w[at + 1, :, c], preferred_element_type=jnp.float32)
                value = (jax.nn.gelu(g) * u).astype(jnp.bfloat16)
                for k in range(TILE // some):
                    start = j * TILE + k * some
                    if part:
                        start = (j * (TILE // some) + k) * quarter + (part - 1) * some
                    to = pl.ds(pl.multiple_of(start, some), some)
                    piece = value[:, k * some : (k + 1) * some]
                    hid[at // 2, slot, 0, :, to] = piece[:half]
                    hid[at // 2, slot, 1, :, to] = piece[half:]
            return 0

        lax.fori_loop(first // 2, last // 2, pair, 0)

    def down(item, stage, loads):
        slot, t, _, sends = steps[item]
        for r, n, part in loads:
            load_copy(r, n, part).wait()
        out = spare(stage)
        unit = [i for i, u in enumerate(UNITS) if slot in (u[0][0], u[1][0])]

        def hidden(i):
            if len(unit) == 1:
                return hid[i, unit[0]].reshape(rows, ff)
            which = [slot == UNITS[unit[0]][k][0] for k in (0, 1)].index(True)
            return hid[i, pl.ds(unit[0], 2), which].reshape(rows, ff)

        def tile(j, _):
            c = pl.ds(pl.multiple_of(j * TILE, TILE), TILE)
            at = t * third + j * TILE
            right = at // wide
            k = pl.ds(pl.multiple_of(right * ff, TILE), ff)
            c_in = pl.ds(pl.multiple_of(at - right * wide, TILE), TILE)
            term = jnp.dot(hidden(0), w[0, k, c_in], preferred_element_type=jnp.float32)
            term += jnp.dot(hidden(1), w[1, k, c_in], preferred_element_type=jnp.float32)
            for r, _, part in loads:
                if part == 0:
                    term = term + load_ref(r)[:, c].astype(jnp.float32)
            for side_, rs in ((1, slice(0, half)), (-1, slice(half, rows))):
                value = term[rs]
                for r, _, part in loads:
                    if part == side_:
                        value = value + load_ref(r)[rs, c].astype(jnp.float32)
                out[rs, c] = value.astype(jnp.bfloat16)
            return 0

        lax.fori_loop(0, third // TILE, tile, 0)
        for n, _, _, _ in sends:
            slot_of[n] = stage
            staged(n).start()
        if not sends:
            result_copy(t, stage).start()

    def result_copy(t, stage):
        return pltpu.make_async_copy(spare(stage), y_ref.at[:, pl.ds(t * third, third)], os.at[t])

    finished, result_stage, brought = set(), {}, set()

    def need(part):
        if part not in brought:
            brought.add(part)
            for copy in bring(part):
                copy.wait()

    def run(action):
        kind = action[0]
        if kind == "wait":
            n = action[1]
            (moving(n) if n in plan else leaving(n, landing(n))).wait_recv()
        elif kind == "go":
            moving(action[1]).start()
        elif kind == "fetch":
            b = action[2]
            (first, _), (second, part) = UNITS[action[1]]
            if first == second:
                pltpu.make_async_copy(block(first), xbuf.at[b], xs.at[b]).start()
            else:
                for slot, to in ((first, 1), (second, -1)):
                    source = block(slot).at[span(part)]
                    pltpu.make_async_copy(source, xbuf.at[b, span(to)], xs.at[b]).start()
        elif kind == "bring":
            for copy in bring(action[1]):
                copy.start()
        elif kind == "load":
            load_copy(*action[1:]).start()
        elif kind == "sent":
            staged(action[1]).wait_send()
            finished.add(action[1])
        else:
            item, stage, loads = action[1:]
            if item[0] == "F":
                result_stage[item[1]] = stage
            need(4)
            need(5 + steps[item][1])
            down(item, stage, loads)

    before, order = [[]], []
    for action in actions:
        if action[0] == "gate":
            before.append([])
            order.append(action)
        else:
            before[-1].append(action)
    rest = before.pop()

    own = [pltpu.make_async_copy(a, w.at[i], ws.at[i]) for i, a in enumerate((wg_ref, wu_ref))]
    for action in before[0]:
        run(action)
    for copy in own:
        copy.start()
    for copy in own:
        copy.wait()

    done = 0
    for part, a, b in GATES:
        if part and part not in brought:
            for action in before[done]:
                run(action)
            before[done] = []
            need(part)

        def step(s, _, part=part, a=a, done=done, b=b):
            for k in range(a, b):
                todo = before[done + k - a] if done + k - a else []
                if todo:

                    @pl.when(s == k)
                    def _(todo=todo):
                        for action in todo:
                            run(action)

            gate_tiles(part, s, lax.rem(s + (done - a), 2))
            return 0

        lax.fori_loop(a, b, step, 0)
        done += b - a
    for action in rest:
        run(action)
    for n in plan:
        moving(n).wait_send()
    for n in sum_id:
        if n not in finished:
            staged(n).wait_send()
    for t in (0, 1, 2):
        result_copy(t, result_stage[t]).wait()


def solution(mesh):
    side = math.isqrt(mesh.shape["tp"])

    def step(x, w_gate, w_up, w_down):
        rows, dim = x.shape
        ff = w_gate.shape[1]
        half, third, quarter = rows // 2, dim // 3, ff // 4
        moves = len(transfers())
        leaves = sum(len(s[3]) for s in sums().values())
        bf16 = jnp.bfloat16
        anywhere = pl.BlockSpec(memory_space=pl.ANY)
        shapes = [
            (rows, dim),
            (7, rows, dim),
            (2, half, dim),
            (3, 2, 2, 2, dim, quarter // 3),
            (3, 2, 2, quarter, third),
            (5, 2, half, third),
            (5, 2, rows, third),
            (6, 2, half, third),
            (6, 2, half, third),
        ]
        return pl.pallas_call(
            functools.partial(kernel, side),
            out_shape=[jax.ShapeDtypeStruct(shape, bf16) for shape in shapes],
            in_specs=[anywhere] * 4,
            out_specs=[anywhere] * len(shapes),
            scratch_shapes=[
                pltpu.VMEM((4, dim, ff), bf16),
                pltpu.VMEM((2, 8, 2, half, ff), bf16),
                pltpu.VMEM((2, rows, dim), bf16),
                pltpu.VMEM((EARLY, rows, third), bf16),
                pltpu.SemaphoreType.DMA((moves,)),
                pltpu.SemaphoreType.DMA((moves,)),
                pltpu.SemaphoreType.DMA((leaves,)),
                pltpu.SemaphoreType.DMA((leaves,)),
                pltpu.SemaphoreType.DMA((44,)),
                pltpu.SemaphoreType.DMA((2,)),
                pltpu.SemaphoreType.DMA((LOADS,)),
                pltpu.SemaphoreType.DMA((3,)),
            ],
            compiler_params=pltpu.CompilerParams(
                collective_id=0, has_side_effects=True, vmem_limit_bytes=66_900_000
            ),
        )(x, w_gate, w_up, w_down)[0]

    return jax.shard_map(
        step,
        mesh=mesh,
        in_specs=(P(("dp", "tp"), None), P(None, "tp"), P(None, "tp"), P("tp", None)),
        out_specs=P(("dp", "tp"), None),
        check_vma=False,
    )


if __name__ == "__main__":
    acts, end, links = schedule()
    for a in acts:
        print(a)
    print(len(acts), end, links)
```

```python
import functools
import math

import jax
import jax.numpy as jnp
from jax import lax
from jax.experimental import pallas as pl
from jax.experimental.pallas import tpu as pltpu
from jax.sharding import PartitionSpec as P

MESH = pl.DeviceIdType.MESH
TILE = 256
EARLY = 4
STAGE = 12
LOADS = 8

HALF_US, HOP_US, LOAD_US, DOWN_US, CORE_US = 23.4, 2.0, 2.0, 3.2, 2.0
GATE_US = (7.4, 2.5, 2.5, 2.5)

BLOCKS = [(0, 0), (0, 1), (0, -1), (0, 2), (2, 0), (2, 1), (2, -1), (2, 2)]
SLOT = {b: i for i, b in enumerate(BLOCKS)}
UNITS = [
    ((0, 1), (0, -1)), ((1, 1), (2, 1)), ((1, -1), (2, -1)), ((3, 1), (3, -1)),
    ((4, 1), (4, -1)), ((5, 1), (6, 1)), ((5, -1), (6, -1)), ((7, 1), (7, -1)),
]
GATES = [
    (0, 0, 5), (1, 0, 4), (0, 5, 6), (1, 4, 7), (2, 0, 1), (0, 6, 7), (2, 1, 8), (1, 7, 8),
    (0, 7, 8), (3, 0, 8),
]
STEPS = [
    ("A", 0, 2), ("B", 0, 0, -1), ("B", 0, 0, 1), ("X", 2), ("X", -1), ("B", 0, 2, -1),
    ("B", 0, 2, 1), ("A", 1, 2), ("X", 1), ("A", 1, 0), ("C", 0), ("A", 2, 0),
    ("X", 0), ("B", 1, 2, -1), ("B", 1, 2, 1), ("B", 2, 0, 1), ("B", 2, 0, -1), ("B", 1, 0, -1),
    ("C", 1), ("B", 1, 0, 1), ("F", 0), ("F", 2), ("S",),
]
EARLY_STEPS = [(("G", 3, 4), ("A", 0, 0))]
LAST = 1
PIECE = 0.7273
ORDER = ("x1", "g1", "x2", "u1", "u2", "g2", "g3", "u3", "d0", "d2", "d1")
WEIGHTS = [w for w in ORDER if w[0] != "x"]


def transfers():
    plan = {}
    for i, w in enumerate(ORDER):
        for d in (1, -1):
            if w == "x1":
                plan["x1", d] = (0, d, 1.0, [], None)
                for part in (1, -1):
                    plan["y1", 0, d, part] = (1, d, 1.0, [], None)
            elif w == "x2":
                plan["x2", d] = (0, d, 1.0, [("x1", d)], None)
                plan["y2", 0, d] = (1, d, 1.0, [("y1", 0, d, d)], None)
            else:
                plan[w, d] = (0, d, PIECE, [], ("x2", d) if "x2" in ORDER[:i] else None)
    for d in (1, -1):
        for w in WEIGHTS:
            plan["over", w, d] = (2, 0, PIECE, [(w, d)], None)
        for part in (1, -1):
            plan["y1", 2, d, part] = (1, d, 1.0, [("x2", part)], None)
        plan["y2", 2, d] = (1, d, 1.0, [("y1", 2, d, d)], None)
        for t in (0, 1):
            plan["r2", t, 0, d] = (0, d, 1 / 3, [("r1", t, 0, d)], None)
        for dy in (2, 1, -1, 0):
            plan["r2", 2, dy, d] = (0, d, 1 / 3, [("r1", 2, dy, d)], None)
    return plan


def pieces_of(unit):
    names = []
    for slot, part in UNITS[unit]:
        across, dy = BLOCKS[slot]
        if dy == 0:
            names += [("x2", part)] if across else []
        elif dy == 2:
            names.append(("y2", across, part))
        else:
            names.append(("y1", across, -dy, part))
    return names


def weight_names(part):
    names = (f"g{part}", f"u{part}") if part < 4 else (f"d{part - 5}",)
    return [n for w in names for d in (1, -1) for n in ((w, d), ("over", w, d))]


def sums():
    steps = {}
    both = lambda t, e: [(("B", t, e, 1), 0), (("B", t, e, -1), 0)]
    over = lambda t, dy: [(("r2", t, dy, 1), 1), (("r2", t, dy, -1), -1)]
    for t in (0, 1):
        for e in (2, 0):
            steps["A", t, e] = (SLOT[e, 2], t, [], [(("A", t, e, d), 1, d, d) for d in (1, -1)])
            for d in (1, -1):
                steps["B", t, e, d] = (SLOT[e, d], t, [(("A", t, e, d), d)], [(("B", t, e, d), 1, d, 0)])
        steps["C", t] = (SLOT[2, 0], t, both(t, 2), [(("r1", t, 0, d), 0, d, d) for d in (1, -1)])
    for dy in (2, 1, -1, 0):
        steps["X", dy] = (SLOT[2, dy], 2, [], [(("r1", 2, dy, d), 0, d, d) for d in (1, -1)])
    steps["A", 2, 0] = (SLOT[0, 2], 2, over(2, 2), [(("A", 2, 0, d), 1, d, d) for d in (1, -1)])
    for d in (1, -1):
        loads = over(2, d) + [(("A", 2, 0, d), d)]
        steps["B", 2, 0, d] = (SLOT[0, d], 2, loads, [(("B", 2, 0, d), 1, d, 0)])
    steps["S",] = (SLOT[0, 0], LAST, [], [])
    for t in {0, 1, 2} - {LAST}:
        steps["F", t] = (SLOT[0, 0], t, both(t, 0) + over(t, 0), [])
    return steps


def sequence():
    seq = [("G", part, i) for part, a, b in GATES for i in range(a, b)]
    for at, item in EARLY_STEPS:
        seq.insert(seq.index(at) + 1, item)
    return seq + STEPS


def schedule():
    plan, steps = transfers(), sums()
    seq = sequence()
    link, arrival, actions = {}, {}, []
    waited, issued, loaded, ready, brought = set(), set(), {}, {}, {}
    now = 0.0

    def send(name, axis, d, size):
        start = max(now, link.get((axis, d), 0.0))
        link[axis, d] = start + size * (CORE_US if axis == 2 else HALF_US)
        arrival[name] = link[axis, d] + HOP_US

    def wait(names):
        for name in names:
            if name not in waited:
                waited.add(name)
                actions.append(("wait", name))

    def here(names):
        return all(n in arrival and arrival[n] <= now for n in names)

    free = list(range(LOADS))
    stage = [(i, None) for i in range(EARLY)]
    own_left = sum(b - a for part, a, b in GATES if part == 0)
    gates = 1 + max(i for i, item in enumerate(seq) if item[0] == "G")
    at = fetched = 0
    while at < len(seq):
        for name, (axis, d, size, needs, after) in plan.items():
            if name not in issued and here(needs) and (after is None or after in issued):
                issued.add(name)
                wait(needs)
                actions.append(("go", name))
                send(name, axis, d, size)
        for part in (1, 2, 3, 4, 5, 6, 7):
            if part not in brought:
                names = [] if part == 4 else weight_names(part)
                if here(names) and not (part >= 4 and own_left):
                    wait(names)
                    actions.append(("bring", part))
                    brought[part] = now + 4.0
        for k, item in enumerate(seq[at : at + 3]):
            if item in loaded:
                continue
            if item[0] == "G":
                if k > 1 or not here(pieces_of(item[2])):
                    break
                wait(pieces_of(item[2]))
                actions.append(("fetch", item[2], fetched % 2))
                fetched += 1
                loaded[item], ready[item] = [], now + LOAD_US
            else:
                loads = steps[item][2]
                units = [i for i, u in enumerate(UNITS) if steps[item][0] in (u[0][0], u[1][0])]
                if any(("G", part, i) in seq[at:] for part in range(4) for i in units):
                    break
                if (loads and at < gates) or len(loads) > len(free) or not here([n for n, _ in loads]):
                    break
                wait([n for n, _ in loads])
                taken = []
                for n, rows in loads:
                    taken.append((free.pop(0), n, rows))
                    actions.append(("load", *taken[-1]))
                loaded[item], ready[item] = taken, (now + LOAD_US if loads else now)
        item = seq[at]
        parts = ([item[1]] if item[1] else []) if item[0] == "G" else [4, 5 + steps[item][1]]
        if item in loaded and ready[item] <= now and all(brought.get(q, 1e9) <= now for q in parts):
            if item[0] == "G":
                actions.append(("gate", item[1], item[2]))
                now += GATE_US[item[1]]
                own_left -= item[1] == 0
            else:
                slot, before = stage.pop(0) if item[0] != "S" else (None, None)
                for n in before or []:
                    now = max(now, arrival[n])
                    actions.append(("sent", n))
                actions.append(("down", item, slot, loaded[item]))
                now += DOWN_US
                free += [r for r, _, _ in loaded[item]]
                for n, axis, d, rows in steps[item][3]:
                    send(n, axis, d, 1 / 3 if rows else 2 / 3)
                if item[0] != "S":
                    stage.append((slot, [n for n, _, _, _ in steps[item][3]]))
            at += 1
            if at == gates:
                stage = [(EARLY + i, None) for i in range(STAGE)] + stage
            continue
        now = min(t for t in [*arrival.values(), *ready.values(), *brought.values()] if t > now)
    last = [(kind, LAST, 0, d) for kind in ("r2", "B") for d in (1, -1)]
    while not here(last):
        for name, (axis, d, size, needs, after) in plan.items():
            if name not in issued and here(needs):
                issued.add(name)
                wait(needs)
                actions.append(("go", name))
                send(name, axis, d, size)
        if not here(last):
            now = min(t for t in arrival.values() if t > now)
    wait(last)
    return actions, now, max(link.values())


def kernel(
    side, x_ref, wg_ref, wu_ref, wd_ref, y_ref, sum_ref, ag, rl, nb, nd, ta, tb, rr, rf,
    w, hid, xbuf, sbuf, fbuf, ts, tr, ss, sr, ws, xs, ls, os,
):
    rows, dim = x_ref.shape
    ff = wg_ref.shape[1]
    half, wide, third = rows // 2, dim // 2, dim // 3
    quarter = ff // 4
    some = quarter // 3
    me, group = lax.axis_index("tp"), lax.axis_index("dp")
    core = lax.rem(group, 2)
    mx, my = me // side, lax.rem(me, side)

    def peer(axis, d):
        if axis == 0:
            return {"tp": lax.rem(mx + d + side, side) * side + my}
        if axis == 1:
            return {"tp": mx * side + lax.rem(my + d + side, side)}
        return {"dp": group + 1 - 2 * core}

    own = [pltpu.make_async_copy(a, w.at[i], ws.at[i]) for i, a in enumerate((wg_ref, wu_ref))]
    for copy in own:
        copy.start()
    barrier = pltpu.get_barrier_semaphore()
    for axis, d in ((0, 1), (0, -1), (1, 1), (1, -1), (2, 0)):
        pl.semaphore_signal(barrier, inc=1, device_id=peer(axis, d), device_id_type=MESH)
    pl.semaphore_wait(barrier, 5)

    plan, steps = transfers(), sums()
    actions, _, _ = schedule()
    plan_id = {n: i for i, n in enumerate(plan)}
    sum_id, sum_send = {}, {}
    for _, _, _, sends in steps.values():
        for n, axis, d, part in sends:
            sum_id[n] = len(sum_id)
            sum_send[n] = (axis, d, part)

    def way(d):
        return 0 if d == 1 else 1

    def span(part):
        return slice(None) if part == 0 else pl.ds(0 if part == 1 else half, half)

    def block(slot):
        return x_ref if slot == 0 else ag.at[slot - 1]

    def landing(n):
        d = way(n[-1])
        if n[0] == "A":
            return ta.at[n[1] * 2 + n[2] // 2, d]
        if n[0] == "B":
            return tb.at[n[1] * 2 + n[2] // 2, d]
        return (rr if n[0] == "r1" else rf).at[n[1] + n[2] % 4, d]

    def ends(n):
        kind, d = n[0], n[-1]
        if kind == "x1":
            return x_ref.at[span(d)], rl.at[way(d)]
        if kind == "x2":
            return rl.at[way(d)], block(SLOT[2, 0]).at[span(d)]
        if kind == "y1":
            _, e, d, part = n
            return block(SLOT[e, 0]).at[span(part)], block(SLOT[e, -d]).at[span(part)]
        if kind == "y2":
            e = n[1]
            return block(SLOT[e, -d]).at[span(d)], block(SLOT[e, 2]).at[span(d)]
        if kind == "r2":
            return landing(("r1", *n[1:])), landing(n)
        over = kind == "over"
        name = n[1] if over else kind
        number = int(name[1])
        if name[0] == "d":
            buf = nd.at[number, way(d)]
        else:
            buf = nb.at[number - 1, 0 if name[0] == "g" else 1, way(d)]
        if over:
            return buf.at[0], buf.at[1]
        at = (2 * quarter if d == 1 else 0) + quarter * core
        if name[0] == "d":
            start = pl.multiple_of(at, quarter)
            return wd_ref.at[pl.ds(start, quarter), pl.ds(number * third, third)], buf.at[0]
        start = pl.multiple_of(at + (number - 1) * some, some)
        return (wg_ref if name[0] == "g" else wu_ref).at[:, pl.ds(start, some)], buf.at[0]

    def moving(n):
        axis, d = plan[n][:2]
        source, target = ends(n)
        return pltpu.make_async_remote_copy(
            src_ref=source, dst_ref=target, send_sem=ts.at[plan_id[n]], recv_sem=tr.at[plan_id[n]],
            device_id=peer(axis, d), device_id_type=MESH,
        )

    def spare(i):
        if i < EARLY:
            return sbuf.at[i]
        i -= EARLY
        return w.at[2 + i // 8, pl.ds((i % 8) * rows, rows), pl.ds(0, third)]

    def load_ref(r):
        if r < 4:
            return spare(EARLY + STAGE + r)
        return xbuf.at[r // 2 - 2, :, pl.ds((r % 2) * wide, third)]

    slot_of = {}

    def leaving(n, source):
        axis, d, part = sum_send[n]
        return pltpu.make_async_remote_copy(
            src_ref=source, dst_ref=landing(n), send_sem=ss.at[sum_id[n]], recv_sem=sr.at[sum_id[n]],
            device_id=peer(axis, d), device_id_type=MESH,
        )

    def staged(n):
        return leaving(n, spare(slot_of[n]).at[span(sum_send[n][2])])

    def load_copy(r, n, part):
        return pltpu.make_async_copy(landing(n), load_ref(r).at[span(part)], ls.at[r])

    def bring(part):
        copies = []
        if part == 4:
            for h in (0, 1):
                copies.append((wd_ref.at[:, pl.ds(h * wide, wide)], w.at[0, pl.ds(h * ff, ff)]))
        elif part < 4:
            for p in range(4):
                for i in (0, 1):
                    target = w.at[2 + i, :, pl.ds(((part - 1) * 4 + p) * some, some)]
                    copies.append((nb.at[part - 1, i, p // 2, p % 2], target))
        else:
            t = part - 5
            for h in (0, 1):
                lo, hi = max(t * third, h * wide), min((t + 1) * third, (h + 1) * wide)
                if lo < hi:
                    for p in range(4):
                        source = nd.at[t, p // 2, p % 2, :, pl.ds(lo - t * third, hi - lo)]
                        target = w.at[1, pl.ds(h * ff + p * quarter, quarter), pl.ds(lo - h * wide, hi - lo)]
                        copies.append((source, target))
        base = {1: 2, 2: 10, 3: 18, 4: 26, 5: 28, 6: 32, 7: 40}[part]
        return [pltpu.make_async_copy(s, t, ws.at[base + i]) for i, (s, t) in enumerate(copies)]

    def gate_tiles(part, slot, b):
        pltpu.make_async_copy(x_ref, xbuf.at[b], xs.at[b]).wait()
        first, last = (0, ff // TILE) if part == 0 else (0, 4 * some // TILE)
        at = 2 if part else 0

        def pair(i, _):
            for j in (2 * i, 2 * i + 1):
                c = pl.ds(pl.multiple_of((4 * some * (part - 1) if part else 0) + j * TILE, TILE), TILE)
                g = jnp.dot(xbuf[b], w[at, :, c], preferred_element_type=jnp.float32)
                u = jnp.dot(xbuf[b], w[at + 1, :, c], preferred_element_type=jnp.float32)
                value = (jax.nn.gelu(g) * u).astype(jnp.bfloat16)
                for k in range(TILE // some):
                    start = j * TILE + k * some
                    if part:
                        start = (j * (TILE // some) + k) * quarter + (part - 1) * some
                    to = pl.ds(pl.multiple_of(start, some), some)
                    piece = value[:, k * some : (k + 1) * some]
                    hid[at // 2, slot, 0, :, to] = piece[:half]
                    hid[at // 2, slot, 1, :, to] = piece[half:]
            return 0

        lax.fori_loop(first // 2, last // 2, pair, 0)

    def down(item, stage, loads):
        slot, t, _, sends = steps[item]
        for r, n, part in loads:
            load_copy(r, n, part).wait()
        out = fbuf if stage is None else spare(stage)
        unit = [i for i, u in enumerate(UNITS) if slot in (u[0][0], u[1][0])]

        def hidden(i):
            if len(unit) == 1:
                return hid[i, unit[0]].reshape(rows, ff)
            which = [slot == UNITS[unit[0]][k][0] for k in (0, 1)].index(True)
            return hid[i, pl.ds(unit[0], 2), which].reshape(rows, ff)

        def tile(j, _):
            c = pl.ds(pl.multiple_of(j * TILE, TILE), TILE)
            at = t * third + j * TILE
            right = at // wide
            k = pl.ds(pl.multiple_of(right * ff, TILE), ff)
            c_in = pl.ds(pl.multiple_of(at - right * wide, TILE), TILE)
            term = jnp.dot(hidden(0), w[0, k, c_in], preferred_element_type=jnp.float32)
            term += jnp.dot(hidden(1), w[1, k, c_in], preferred_element_type=jnp.float32)
            for r, _, part in loads:
                if part == 0:
                    term = term + load_ref(r)[:, c].astype(jnp.float32)
            if stage is None:
                out[:, c] = term
                return 0
            for side_, rs in ((1, slice(0, half)), (-1, slice(half, rows))):
                value = term[rs]
                for r, _, part in loads:
                    if part == side_:
                        value = value + load_ref(r)[rs, c].astype(jnp.float32)
                out[rs, c] = value.astype(jnp.bfloat16)
            return 0

        lax.fori_loop(0, third // TILE, tile, 0)
        for n, _, _, _ in sends:
            slot_of[n] = stage
            staged(n).start()
        if not sends:
            result_copy(t, stage).start()

    def result_copy(t, stage):
        if stage is None:
            return pltpu.make_async_copy(fbuf, sum_ref, os.at[t])
        return pltpu.make_async_copy(spare(stage), y_ref.at[:, pl.ds(t * third, third)], os.at[t])

    finished, result_stage, brought = set(), {}, set()

    def need(part):
        if part not in brought:
            brought.add(part)
            for copy in bring(part):
                copy.wait()

    def run(action):
        kind = action[0]
        if kind == "wait":
            n = action[1]
            (moving(n) if n in plan else leaving(n, landing(n))).wait_recv()
        elif kind == "go":
            moving(action[1]).start()
        elif kind == "fetch":
            b = action[2]
            (first, _), (second, part) = UNITS[action[1]]
            if first == second:
                pltpu.make_async_copy(block(first), xbuf.at[b], xs.at[b]).start()
            else:
                for slot, to in ((first, 1), (second, -1)):
                    source = block(slot).at[span(part)]
                    pltpu.make_async_copy(source, xbuf.at[b, span(to)], xs.at[b]).start()
        elif kind == "bring":
            for copy in bring(action[1]):
                copy.start()
        elif kind == "load":
            load_copy(*action[1:]).start()
        elif kind == "sent":
            staged(action[1]).wait_send()
            finished.add(action[1])
        else:
            item, stage, loads = action[1:]
            if item[0] in "FS":
                result_stage[steps[item][1]] = stage
            need(4)
            need(5 + steps[item][1])
            down(item, stage, loads)

    before, order = [[]], []
    for action in actions:
        if action[0] == "gate":
            before.append([])
            order.append(action)
        else:
            before[-1].append(action)
    rest = before.pop()

    for action in before[0]:
        run(action)
    for copy in own:
        copy.wait()

    done = 0
    for part, a, b in GATES:
        if part and part not in brought:
            for action in before[done]:
                run(action)
            before[done] = []
            need(part)

        def step(s, _, part=part, a=a, done=done, b=b):
            for k in range(a, b):
                todo = before[done + k - a] if done + k - a else []
                if todo:

                    @pl.when(s == k)
                    def _(todo=todo):
                        for action in todo:
                            run(action)

            gate_tiles(part, s, lax.rem(s + (done - a), 2))
            return 0

        lax.fori_loop(a, b, step, 0)
        done += b - a
    for action in rest:
        run(action)
    for n in plan:
        moving(n).wait_send()
    for n in sum_id:
        if n not in finished:
            staged(n).wait_send()
    for t in (0, 1, 2):
        result_copy(t, result_stage[t]).wait()


def finish(part_ref, sum_ref, along_ref, last_ref, y_ref):
    third = sum_ref.shape[1]
    for t in (0, 1, 2):
        c = slice(t * third, (t + 1) * third)
        if t == LAST:
            value = sum_ref[...]
            for piece in (along_ref[0, 0], along_ref[0, 1], last_ref[0, 0]):
                value = value + piece.astype(jnp.float32)
            y_ref[:, c] = value.astype(jnp.bfloat16)
        else:
            y_ref[:, c] = part_ref[:, c]


def solution(mesh):
    side = math.isqrt(mesh.shape["tp"])

    def step(x, w_gate, w_up, w_down):
        rows, dim = x.shape
        ff = w_gate.shape[1]
        half, third, quarter = rows // 2, dim // 3, ff // 4
        moves = len(transfers())
        leaves = sum(len(s[3]) for s in sums().values())
        bf16 = jnp.bfloat16
        anywhere = pl.BlockSpec(memory_space=pl.ANY)
        shapes = [
            (rows, dim),
            (7, rows, dim),
            (2, half, dim),
            (3, 2, 2, 2, dim, quarter // 3),
            (3, 2, 2, quarter, third),
            (5, 2, half, third),
            (5, 2, rows, third),
            (6, 2, half, third),
            (6, 2, half, third),
        ]
        kinds = [jax.ShapeDtypeStruct(shape, bf16) for shape in shapes]
        kinds.insert(1, jax.ShapeDtypeStruct((rows, third), jnp.float32))
        outs = pl.pallas_call(
            functools.partial(kernel, side),
            out_shape=kinds,
            in_specs=[anywhere] * 4,
            out_specs=[anywhere] * len(kinds),
            scratch_shapes=[
                pltpu.VMEM((4, dim, ff), bf16),
                pltpu.VMEM((2, 8, 2, half, ff), bf16),
                pltpu.VMEM((2, rows, dim), bf16),
                pltpu.VMEM((EARLY, rows, third), bf16),
                pltpu.VMEM((rows, third), jnp.float32),
                pltpu.SemaphoreType.DMA((moves,)),
                pltpu.SemaphoreType.DMA((moves,)),
                pltpu.SemaphoreType.DMA((leaves,)),
                pltpu.SemaphoreType.DMA((leaves,)),
                pltpu.SemaphoreType.DMA((44,)),
                pltpu.SemaphoreType.DMA((2,)),
                pltpu.SemaphoreType.DMA((LOADS,)),
                pltpu.SemaphoreType.DMA((3,)),
            ],
            compiler_params=pltpu.CompilerParams(
                collective_id=0, has_side_effects=True, vmem_limit_bytes=66_900_000
            ),
        )(x, w_gate, w_up, w_down)
        return pl.pallas_call(
            finish,
            grid=(2,),
            out_shape=jax.ShapeDtypeStruct((rows, dim), bf16),
            in_specs=[
                pl.BlockSpec((half, dim), lambda k: (k, 0)),
                pl.BlockSpec((half, third), lambda k: (k, 0)),
                pl.BlockSpec((1, 2, half, third), lambda k: (2 * LAST, 0, k, 0)),
                pl.BlockSpec((1, 1, half, third), lambda k: (LAST, k, 0, 0)),
            ],
            out_specs=pl.BlockSpec((half, dim), lambda k: (k, 0)),
        )(outs[0], outs[1], outs[-3], outs[-1])

    return jax.shard_map(
        step,
        mesh=mesh,
        in_specs=(P(("dp", "tp"), None), P(None, "tp"), P(None, "tp"), P("tp", None)),
        out_specs=P(("dp", "tp"), None),
        check_vma=False,
    )


if __name__ == "__main__":
    acts, end, links = schedule()
    for a in acts:
        print(a)
    print(len(acts), end, links)
```

```python
import functools
import math

import jax
import jax.numpy as jnp
from jax import lax
from jax.experimental import pallas as pl
from jax.experimental.pallas import tpu as pltpu
from jax.sharding import PartitionSpec as P

MESH = pl.DeviceIdType.MESH
TILE = 256
EARLY = 4
STAGE = 12
EARLY_LOADS = 2
LOADS = 8

HALF_US, HOP_US, LOAD_US, DOWN_US, CORE_US = 23.3, 2.2, 2.0, 3.2, 2.0
GATE_US = (7.4, 2.5, 2.5, 2.5)

BLOCKS = [(0, 0), (0, 1), (0, -1), (0, 2), (2, 0), (2, 1), (2, -1), (2, 2)]
SLOT = {b: i for i, b in enumerate(BLOCKS)}
UNITS = [
    ((0, 1), (0, -1)), ((1, 1), (2, 1)), ((1, -1), (2, -1)), ((3, 1), (3, -1)),
    ((4, 1), (4, -1)), ((5, 1), (6, 1)), ((5, -1), (6, -1)), ((7, 1), (7, -1)),
]
GATES = [
    (0, 0, 6), (2, 4, 1), (2, 6, 4), (1, 6, 4), (1, 0, 5), (2, 1, -1), (0, 7, 5), (2, 7, 8),
    (1, 7, 8), (3, 7, -1),
]
STEPS = [
    ("X", 1), ("A", 1, 0), ("X", -1), ("A", 2, 0), ("B", 1, 2, 1), ("B", 1, 2, -1),
    ("X", 0), ("B", 0, 0, -1), ("B", 0, 0, 1), ("B", 2, 0, 1), ("C", 0), ("C", 1),
    ("B", 2, 0, -1), ("B", 1, 0, 1), ("B", 1, 0, -1), ("F", 2), ("S",), ("F", 0),
]
EARLY_STEPS = [(("G", 3, 7), ("A", 0, 2)), (("G", 3, 3), ("A", 0, 0)), (("A", 0, 0), ("B", 0, 2, -1)), (("B", 0, 2, -1), ("B", 0, 2, 1)), (("B", 0, 2, 1), ("X", 2)), (("G", 3, 1), ("A", 1, 2))]
LAST = 1
PIECE = 0.7273
ORDER = ("x1", "g2", "x2", "u2", "u1", "g1", "g3", "u3", "d0", "d2", "d1")
WEIGHTS = [w for w in ORDER if w[0] != "x"]


def units_of(a, b):
    return list(range(a, b, 1 if b > a else -1))


def transfers():
    plan = {}
    for i, w in enumerate(ORDER):
        for d in (1, -1):
            if w == "x1":
                plan["x1", d] = (0, d, 1.0, [], None)
                for part in (1, -1):
                    plan["y1", 0, d, part] = (1, d, 1.0, [], None)
            elif w == "x2":
                plan["x2", d] = (0, d, 1.0, [("x1", d)], None)
                plan["y2", 0, d] = (1, d, 1.0, [("y1", 0, d, d)], None)
            else:
                plan[w, d] = (0, d, PIECE, [], ("x2", d) if "x2" in ORDER[:i] else None)
    for d in (1, -1):
        for w in WEIGHTS:
            plan["over", w, d] = (2, 0, PIECE, [(w, d)], None)
        for part in (1, -1):
            plan["y1", 2, d, part] = (1, d, 1.0, [("x2", part)], None)
        plan["y2", 2, d] = (1, d, 1.0, [("y1", 2, d, d)], None)
        for t in (0, 1):
            plan["r2", t, 0, d] = (0, d, 1 / 3, [("r1", t, 0, d)], None)
        for dy in (2, 1, -1, 0):
            plan["r2", 2, dy, d] = (0, d, 1 / 3, [("r1", 2, dy, d)], None)
    return plan


def pieces_of(unit):
    names = []
    for slot, part in UNITS[unit]:
        across, dy = BLOCKS[slot]
        if dy == 0:
            names += [("x2", part)] if across else []
        elif dy == 2:
            names.append(("y2", across, part))
        else:
            names.append(("y1", across, -dy, part))
    return names


def weight_names(part):
    names = (f"g{part}", f"u{part}") if part < 4 else (f"d{part - 5}",)
    return [n for w in names for d in (1, -1) for n in ((w, d), ("over", w, d))]


def sums():
    steps = {}
    both = lambda t, e: [(("B", t, e, 1), 0), (("B", t, e, -1), 0)]
    over = lambda t, dy: [(("r2", t, dy, 1), 1), (("r2", t, dy, -1), -1)]
    for t in (0, 1):
        for e in (2, 0):
            steps["A", t, e] = (SLOT[e, 2], t, [], [(("A", t, e, d), 1, d, d) for d in (1, -1)])
            for d in (1, -1):
                steps["B", t, e, d] = (SLOT[e, d], t, [(("A", t, e, d), d)], [(("B", t, e, d), 1, d, 0)])
        steps["C", t] = (SLOT[2, 0], t, both(t, 2), [(("r1", t, 0, d), 0, d, d) for d in (1, -1)])
    for dy in (2, 1, -1, 0):
        steps["X", dy] = (SLOT[2, dy], 2, [], [(("r1", 2, dy, d), 0, d, d) for d in (1, -1)])
    steps["A", 2, 0] = (SLOT[0, 2], 2, over(2, 2), [(("A", 2, 0, d), 1, d, d) for d in (1, -1)])
    for d in (1, -1):
        loads = over(2, d) + [(("A", 2, 0, d), d)]
        steps["B", 2, 0, d] = (SLOT[0, d], 2, loads, [(("B", 2, 0, d), 1, d, 0)])
    steps["S",] = (SLOT[0, 0], LAST, [], [])
    for t in {0, 1, 2} - {LAST}:
        steps["F", t] = (SLOT[0, 0], t, both(t, 0) + over(t, 0), [])
    return steps


def sequence():
    seq = [("G", part, i) for part, a, b in GATES for i in units_of(a, b)]
    for at, item in EARLY_STEPS:
        seq.insert(seq.index(at) + 1, item)
    return seq + STEPS


def schedule():
    plan, steps = transfers(), sums()
    seq = sequence()
    link, arrival, actions = {}, {}, []
    waited, issued, loaded, ready, brought = set(), set(), {}, {}, {}
    now = 0.0

    def send(name, axis, d, size):
        start = max(now, link.get((axis, d), 0.0))
        link[axis, d] = start + size * (CORE_US if axis == 2 else HALF_US)
        arrival[name] = link[axis, d] + HOP_US

    def wait(names):
        for name in names:
            if name not in waited:
                waited.add(name)
                actions.append(("wait", name))

    def here(names):
        return all(n in arrival and arrival[n] <= now for n in names)

    free = list(range(LOADS, LOADS + EARLY_LOADS))
    stage = [(i, None) for i in range(EARLY)]
    own_left = sum(abs(b - a) for part, a, b in GATES if part == 0)
    gates = 1 + max(i for i, item in enumerate(seq) if item[0] == "G")
    at = fetched = 0
    while at < len(seq):
        for name, (axis, d, size, needs, after) in plan.items():
            if name not in issued and here(needs) and (after is None or after in issued):
                issued.add(name)
                wait(needs)
                actions.append(("go", name))
                send(name, axis, d, size)
        for part in (1, 2, 3, 4, 5, 6, 7):
            if part not in brought:
                names = [] if part == 4 else weight_names(part)
                if here(names) and not (part >= 4 and own_left):
                    wait(names)
                    actions.append(("bring", part))
                    brought[part] = now + 4.0
        for k, item in enumerate(seq[at : at + 3]):
            if item in loaded:
                continue
            if item[0] == "G":
                if k > 1 or not here(pieces_of(item[2])):
                    break
                wait(pieces_of(item[2]))
                actions.append(("fetch", item[2], fetched % 2))
                fetched += 1
                loaded[item], ready[item] = [], now + LOAD_US
            else:
                loads = steps[item][2]
                units = [i for i, u in enumerate(UNITS) if steps[item][0] in (u[0][0], u[1][0])]
                if any(("G", part, i) in seq[at:] for part in range(4) for i in units):
                    break
                if len(loads) > len(free) or not here([n for n, _ in loads]):
                    break
                wait([n for n, _ in loads])
                taken = []
                for n, rows in loads:
                    taken.append((free.pop(0), n, rows))
                    actions.append(("load", *taken[-1]))
                loaded[item], ready[item] = taken, (now + LOAD_US if loads else now)
        item = seq[at]
        parts = ([item[1]] if item[1] else []) if item[0] == "G" else [4, 5 + steps[item][1]]
        if item in loaded and ready[item] <= now and all(brought.get(q, 1e9) <= now for q in parts):
            if item[0] == "G":
                actions.append(("gate", item[1], item[2]))
                now += GATE_US[item[1]]
                own_left -= item[1] == 0
            else:
                slot, before = stage.pop(0) if item[0] != "S" else (None, None)
                for n in before or []:
                    now = max(now, arrival[n])
                    actions.append(("sent", n))
                actions.append(("down", item, slot, loaded[item]))
                now += DOWN_US
                free += [r for r, _, _ in loaded[item]]
                for n, axis, d, rows in steps[item][3]:
                    send(n, axis, d, 1 / 3 if rows else 2 / 3)
                if item[0] != "S":
                    stage.append((slot, [n for n, _, _, _ in steps[item][3]]))
            at += 1
            if at == gates:
                stage = [(EARLY + i, None) for i in range(STAGE)] + stage
                free = list(range(LOADS)) + free
            continue
        now = min(t for t in [*arrival.values(), *ready.values(), *brought.values()] if t > now)
    last = [(kind, LAST, 0, d) for kind in ("r2", "B") for d in (1, -1)]
    while not here(last):
        for name, (axis, d, size, needs, after) in plan.items():
            if name not in issued and here(needs):
                issued.add(name)
                wait(needs)
                actions.append(("go", name))
                send(name, axis, d, size)
        if not here(last):
            now = min(t for t in arrival.values() if t > now)
    wait(last)
    return actions, now, max(link.values())


def kernel(
    side, x_ref, wg_ref, wu_ref, wd_ref, y_ref, sum_ref, ag, rl, nb, nd, ta, tb, rr, rf,
    w, hid, xbuf, sbuf, fbuf, lbuf, ts, tr, ss, sr, ws, xs, ls, os,
):
    rows, dim = x_ref.shape
    ff = wg_ref.shape[1]
    half, wide, third = rows // 2, dim // 2, dim // 3
    quarter = ff // 4
    some = quarter // 3
    me, group = lax.axis_index("tp"), lax.axis_index("dp")
    core = lax.rem(group, 2)
    mx, my = me // side, lax.rem(me, side)

    def peer(axis, d):
        if axis == 0:
            return {"tp": lax.rem(mx + d + side, side) * side + my}
        if axis == 1:
            return {"tp": mx * side + lax.rem(my + d + side, side)}
        return {"dp": group + 1 - 2 * core}

    own = [pltpu.make_async_copy(a, w.at[i], ws.at[i]) for i, a in enumerate((wg_ref, wu_ref))]
    for copy in own:
        copy.start()
    barrier = pltpu.get_barrier_semaphore()
    for axis, d in ((0, 1), (0, -1), (1, 1), (1, -1), (2, 0)):
        pl.semaphore_signal(barrier, inc=1, device_id=peer(axis, d), device_id_type=MESH)
    pl.semaphore_wait(barrier, 5)

    plan, steps = transfers(), sums()
    actions, _, _ = schedule()
    plan_id = {n: i for i, n in enumerate(plan)}
    sum_id, sum_send = {}, {}
    for _, _, _, sends in steps.values():
        for n, axis, d, part in sends:
            sum_id[n] = len(sum_id)
            sum_send[n] = (axis, d, part)

    def way(d):
        return 0 if d == 1 else 1

    def span(part):
        return slice(None) if part == 0 else pl.ds(0 if part == 1 else half, half)

    def block(slot):
        return x_ref if slot == 0 else ag.at[slot - 1]

    def landing(n):
        d = way(n[-1])
        if n[0] == "A":
            return ta.at[n[1] * 2 + n[2] // 2, d]
        if n[0] == "B":
            return tb.at[n[1] * 2 + n[2] // 2, d]
        return (rr if n[0] == "r1" else rf).at[n[1] + n[2] % 4, d]

    def ends(n):
        kind, d = n[0], n[-1]
        if kind == "x1":
            return x_ref.at[span(d)], rl.at[way(d)]
        if kind == "x2":
            return rl.at[way(d)], block(SLOT[2, 0]).at[span(d)]
        if kind == "y1":
            _, e, d, part = n
            return block(SLOT[e, 0]).at[span(part)], block(SLOT[e, -d]).at[span(part)]
        if kind == "y2":
            e = n[1]
            return block(SLOT[e, -d]).at[span(d)], block(SLOT[e, 2]).at[span(d)]
        if kind == "r2":
            return landing(("r1", *n[1:])), landing(n)
        over = kind == "over"
        name = n[1] if over else kind
        number = int(name[1])
        if name[0] == "d":
            buf = nd.at[number, way(d)]
        else:
            buf = nb.at[number - 1, 0 if name[0] == "g" else 1, way(d)]
        if over:
            return buf.at[0], buf.at[1]
        at = (2 * quarter if d == 1 else 0) + quarter * core
        if name[0] == "d":
            start = pl.multiple_of(at, quarter)
            return wd_ref.at[pl.ds(start, quarter), pl.ds(number * third, third)], buf.at[0]
        start = pl.multiple_of(at + (number - 1) * some, some)
        return (wg_ref if name[0] == "g" else wu_ref).at[:, pl.ds(start, some)], buf.at[0]

    def moving(n):
        axis, d = plan[n][:2]
        source, target = ends(n)
        return pltpu.make_async_remote_copy(
            src_ref=source, dst_ref=target, send_sem=ts.at[plan_id[n]], recv_sem=tr.at[plan_id[n]],
            device_id=peer(axis, d), device_id_type=MESH,
        )

    def spare(i):
        if i < EARLY:
            return sbuf.at[i]
        i -= EARLY
        return w.at[2 + i // 8, pl.ds((i % 8) * rows, rows), pl.ds(0, third)]

    def load_ref(r):
        if r >= LOADS:
            return lbuf.at[r - LOADS]
        if r < 4:
            return spare(EARLY + STAGE + r)
        return xbuf.at[r // 2 - 2, :, pl.ds((r % 2) * wide, third)]

    slot_of = {}

    def leaving(n, source):
        axis, d, part = sum_send[n]
        return pltpu.make_async_remote_copy(
            src_ref=source, dst_ref=landing(n), send_sem=ss.at[sum_id[n]], recv_sem=sr.at[sum_id[n]],
            device_id=peer(axis, d), device_id_type=MESH,
        )

    def staged(n):
        return leaving(n, spare(slot_of[n]).at[span(sum_send[n][2])])

    def load_copy(r, n, part):
        return pltpu.make_async_copy(landing(n), load_ref(r).at[span(part)], ls.at[r])

    def bring(part):
        copies = []
        if part == 4:
            for h in (0, 1):
                copies.append((wd_ref.at[:, pl.ds(h * wide, wide)], w.at[0, pl.ds(h * ff, ff)]))
        elif part < 4:
            for p in range(4):
                for i in (0, 1):
                    target = w.at[2 + i, :, pl.ds(((part - 1) * 4 + p) * some, some)]
                    copies.append((nb.at[part - 1, i, p // 2, p % 2], target))
        else:
            t = part - 5
            for h in (0, 1):
                lo, hi = max(t * third, h * wide), min((t + 1) * third, (h + 1) * wide)
                if lo < hi:
                    for p in range(4):
                        source = nd.at[t, p // 2, p % 2, :, pl.ds(lo - t * third, hi - lo)]
                        target = w.at[1, pl.ds(h * ff + p * quarter, quarter), pl.ds(lo - h * wide, hi - lo)]
                        copies.append((source, target))
        base = {1: 2, 2: 10, 3: 18, 4: 26, 5: 28, 6: 32, 7: 40}[part]
        return [pltpu.make_async_copy(s, t, ws.at[base + i]) for i, (s, t) in enumerate(copies)]

    def gate_tiles(part, slot, b):
        pltpu.make_async_copy(x_ref, xbuf.at[b], xs.at[b]).wait()
        first, last = (0, ff // TILE) if part == 0 else (0, 4 * some // TILE)
        at = 2 if part else 0

        def pair(i, _):
            for j in (2 * i, 2 * i + 1):
                c = pl.ds(pl.multiple_of((4 * some * (part - 1) if part else 0) + j * TILE, TILE), TILE)
                g = jnp.dot(xbuf[b], w[at, :, c], preferred_element_type=jnp.float32)
                u = jnp.dot(xbuf[b], w[at + 1, :, c], preferred_element_type=jnp.float32)
                value = (jax.nn.gelu(g) * u).astype(jnp.bfloat16)
                for k in range(TILE // some):
                    start = j * TILE + k * some
                    if part:
                        start = (j * (TILE // some) + k) * quarter + (part - 1) * some
                    to = pl.ds(pl.multiple_of(start, some), some)
                    piece = value[:, k * some : (k + 1) * some]
                    hid[at // 2, slot, 0, :, to] = piece[:half]
                    hid[at // 2, slot, 1, :, to] = piece[half:]
            return 0

        lax.fori_loop(first // 2, last // 2, pair, 0)

    def down(item, stage, loads):
        slot, t, _, sends = steps[item]
        for r, n, part in loads:
            load_copy(r, n, part).wait()
        out = fbuf if stage is None else spare(stage)
        unit = [i for i, u in enumerate(UNITS) if slot in (u[0][0], u[1][0])]

        def hidden(i):
            if len(unit) == 1:
                return hid[i, unit[0]].reshape(rows, ff)
            which = [slot == UNITS[unit[0]][k][0] for k in (0, 1)].index(True)
            return hid[i, pl.ds(unit[0], 2), which].reshape(rows, ff)

        def tile(j, _):
            c = pl.ds(pl.multiple_of(j * TILE, TILE), TILE)
            at = t * third + j * TILE
            right = at // wide
            k = pl.ds(pl.multiple_of(right * ff, TILE), ff)
            c_in = pl.ds(pl.multiple_of(at - right * wide, TILE), TILE)
            term = jnp.dot(hidden(0), w[0, k, c_in], preferred_element_type=jnp.float32)
            term += jnp.dot(hidden(1), w[1, k, c_in], preferred_element_type=jnp.float32)
            for r, _, part in loads:
                if part == 0:
                    term = term + load_ref(r)[:, c].astype(jnp.float32)
            if stage is None:
                out[:, c] = term
                return 0
            for side_, rs in ((1, slice(0, half)), (-1, slice(half, rows))):
                value = term[rs]
                for r, _, part in loads:
                    if part == side_:
                        value = value + load_ref(r)[rs, c].astype(jnp.float32)
                out[rs, c] = value.astype(jnp.bfloat16)
            return 0

        lax.fori_loop(0, third // TILE, tile, 0)
        for n, _, _, _ in sends:
            slot_of[n] = stage
            staged(n).start()
        if not sends:
            result_copy(t, stage).start()

    def result_copy(t, stage):
        if stage is None:
            return pltpu.make_async_copy(fbuf, sum_ref, os.at[t])
        return pltpu.make_async_copy(spare(stage), y_ref.at[:, pl.ds(t * third, third)], os.at[t])

    finished, result_stage, brought = set(), {}, set()

    def need(part):
        if part not in brought:
            brought.add(part)
            for copy in bring(part):
                copy.wait()

    def run(action):
        kind = action[0]
        if kind == "wait":
            n = action[1]
            (moving(n) if n in plan else leaving(n, landing(n))).wait_recv()
        elif kind == "go":
            moving(action[1]).start()
        elif kind == "fetch":
            b = action[2]
            (first, _), (second, part) = UNITS[action[1]]
            if first == second:
                pltpu.make_async_copy(block(first), xbuf.at[b], xs.at[b]).start()
            else:
                for slot, to in ((first, 1), (second, -1)):
                    source = block(slot).at[span(part)]
                    pltpu.make_async_copy(source, xbuf.at[b, span(to)], xs.at[b]).start()
        elif kind == "bring":
            for copy in bring(action[1]):
                copy.start()
        elif kind == "load":
            load_copy(*action[1:]).start()
        elif kind == "sent":
            staged(action[1]).wait_send()
            finished.add(action[1])
        else:
            item, stage, loads = action[1:]
            if item[0] in "FS":
                result_stage[steps[item][1]] = stage
            need(4)
            need(5 + steps[item][1])
            down(item, stage, loads)

    before, order = [[]], []
    for action in actions:
        if action[0] == "gate":
            before.append([])
            order.append(action)
        else:
            before[-1].append(action)
    rest = before.pop()

    for action in before[0]:
        run(action)
    for copy in own:
        copy.wait()

    done = 0
    for part, a, b in GATES:
        if part and part not in brought:
            for action in before[done]:
                run(action)
            before[done] = []
            need(part)

        def step(s, _, part=part, a=a, done=done, b=b):
            for k in range(abs(b - a)):
                todo = before[done + k] if done + k else []
                if todo:

                    @pl.when(s == k)
                    def _(todo=todo):
                        for action in todo:
                            run(action)

            gate_tiles(part, a + s if b > a else a - s, lax.rem(s + done, 2))
            return 0

        lax.fori_loop(0, abs(b - a), step, 0)
        done += abs(b - a)
    for action in rest:
        run(action)
    for n in plan:
        moving(n).wait_send()
    for n in sum_id:
        if n not in finished:
            staged(n).wait_send()
    for t in (0, 1, 2):
        result_copy(t, result_stage[t]).wait()


def finish(part_ref, sum_ref, along_ref, last_ref, y_ref):
    third = sum_ref.shape[1]
    for t in (0, 1, 2):
        c = slice(t * third, (t + 1) * third)
        if t == LAST:
            value = sum_ref[...]
            for piece in (along_ref[0, 0], along_ref[0, 1], last_ref[0, 0]):
                value = value + piece.astype(jnp.float32)
            y_ref[:, c] = value.astype(jnp.bfloat16)
        else:
            y_ref[:, c] = part_ref[:, c]


def solution(mesh):
    side = math.isqrt(mesh.shape["tp"])

    def step(x, w_gate, w_up, w_down):
        rows, dim = x.shape
        ff = w_gate.shape[1]
        half, third, quarter = rows // 2, dim // 3, ff // 4
        moves = len(transfers())
        leaves = sum(len(s[3]) for s in sums().values())
        bf16 = jnp.bfloat16
        anywhere = pl.BlockSpec(memory_space=pl.ANY)
        shapes = [
            (rows, dim),
            (7, rows, dim),
            (2, half, dim),
            (3, 2, 2, 2, dim, quarter // 3),
            (3, 2, 2, quarter, third),
            (5, 2, half, third),
            (5, 2, rows, third),
            (6, 2, half, third),
            (6, 2, half, third),
        ]
        kinds = [jax.ShapeDtypeStruct(shape, bf16) for shape in shapes]
        kinds.insert(1, jax.ShapeDtypeStruct((rows, third), jnp.float32))
        outs = pl.pallas_call(
            functools.partial(kernel, side),
            out_shape=kinds,
            in_specs=[anywhere] * 4,
            out_specs=[anywhere] * len(kinds),
            scratch_shapes=[
                pltpu.VMEM((4, dim, ff), bf16),
                pltpu.VMEM((2, 8, 2, half, ff), bf16),
                pltpu.VMEM((2, rows, dim), bf16),
                pltpu.VMEM((EARLY, rows, third), bf16),
                pltpu.VMEM((rows, third), jnp.float32),
                pltpu.VMEM((EARLY_LOADS, rows, third), bf16),
                pltpu.SemaphoreType.DMA((moves,)),
                pltpu.SemaphoreType.DMA((moves,)),
                pltpu.SemaphoreType.DMA((leaves,)),
                pltpu.SemaphoreType.DMA((leaves,)),
                pltpu.SemaphoreType.DMA((44,)),
                pltpu.SemaphoreType.DMA((2,)),
                pltpu.SemaphoreType.DMA((LOADS + EARLY_LOADS,)),
                pltpu.SemaphoreType.DMA((3,)),
            ],
            compiler_params=pltpu.CompilerParams(
                collective_id=0, has_side_effects=True, vmem_limit_bytes=66_900_000
            ),
        )(x, w_gate, w_up, w_down)
        return pl.pallas_call(
            finish,
            grid=(2,),
            out_shape=jax.ShapeDtypeStruct((rows, dim), bf16),
            in_specs=[
                pl.BlockSpec((half, dim), lambda k: (k, 0)),
                pl.BlockSpec((half, third), lambda k: (k, 0)),
                pl.BlockSpec((1, 2, half, third), lambda k: (2 * LAST, 0, k, 0)),
                pl.BlockSpec((1, 1, half, third), lambda k: (LAST, k, 0, 0)),
            ],
            out_specs=pl.BlockSpec((half, dim), lambda k: (k, 0)),
        )(outs[0], outs[1], outs[-3], outs[-1])

    return jax.shard_map(
        step,
        mesh=mesh,
        in_specs=(P(("dp", "tp"), None), P(None, "tp"), P(None, "tp"), P("tp", None)),
        out_specs=P(("dp", "tp"), None),
        check_vma=False,
    )


if __name__ == "__main__":
    acts, end, links = schedule()
    for a in acts:
        print(a)
    print(len(acts), end, links)
```
